32 devices in a mesh: stn: 4 (over z), chan: 4 (over y, core), tile: 2 (over x).
Axes of the slice: x: 2, y: 2, z: 4, core: 2. Of those that a mesh axis runs over, the one named last changes fastest.
Arguments:
- model_image: bfloat16 [8, 64, 2048], P('tile', 'stn'), may hold values from -0.005859375 to 0.005859375
- station_beams: float32 [2, 64, 1024], replicated, may hold values from -6 to 6
- subgrid_offsets: int32 [4, 128, 2], P('chan'), may hold values from -4096 to 4064
- subgrid_stations: int32 [128, 2], P(('stn', 'tile')), may hold values from 0 to 63, as said below
- visibility_uv: float32 [2, 128, 512], P(None, ('stn', 'tile'), 'chan'), may hold values from 2 to 30
- observed: float32 [2, 32, 4, 512], P(None, ('stn', 'tile'), 'chan'), may hold values from -3 to 3
- live_counts: int32 [32, 4], P(('stn', 'tile'), 'chan'), may hold values from 1 to 8
Outputs:
- residual: float32 [2, 32, 4, 512], P(None, ('stn', 'tile'), 'chan')
The draws below stay inside these ranges and needn't reach their ends.
Inputs may be any that keep to these rules, and one draw needn't show every extreme that they name: `subgrid_stations`: each row names two different stations. `live_counts`: rows with a time step at or beyond the count carry no data.
All inputs are finite; a program needn't handle non-finite values.
Results may differ from the reference program's by a relative error of at most 0.00071.
Values may be sent and summed in bfloat16 or wider, within the bound.
A program may use at most 64 MiB of HBM per device.

```python
import math
import jax
import jax.numpy as jnp
from jax import lax

SG = 32
NG = 8192
STATIONS = 64
CHAN_GRP = 16
TIMES = 8
TM = 2048
TL = 64
TILES = 8
VROWS = 512
NSUB = 128
N_CHAN = 4


def draw_subgrid_stations(key, part):
    station_key = jax.random.fold_in(key, 11)
    stride_key = jax.random.fold_in(key, 12)
    station_one = jax.random.randint(station_key, (NSUB,), 0, STATIONS, dtype=jnp.int32)
    stride = jax.random.randint(stride_key, (NSUB,), 1, STATIONS, dtype=jnp.int32)
    station_two = jnp.mod(station_one + stride, STATIONS)
    return jnp.stack([station_one, station_two], axis=1)


def with_ends(array, stream_key, smallest, high):
    longest = array.shape.index(max(array.shape))
    spots = []
    for shift in (0, 1):
        where = [jax.random.randint(jax.random.fold_in(stream_key, axis), (), 0, length) for axis, length in enumerate(array.shape)]
        where[longest] = (where[longest] + shift) % array.shape[longest]
        spots.append(tuple(where))
    return array.at[spots[0]].set(smallest).at[spots[1]].set(high)


def block_scale(key, dims, shards, low, high):
    loudness, own = 1.0, jax.random.fold_in(key, 6)
    for axis_at, parts in shards:
        steps = jnp.exp(jax.random.uniform(jax.random.fold_in(own, axis_at), (parts,), jnp.float32, low / len(shards), high / len(shards)))
        loudness = loudness * jnp.repeat(steps, dims[axis_at] // parts).reshape([-1 if axis == axis_at else 1 for axis in range(len(dims))])
    return loudness


def noise(own_key, extent, spread, most, pieces=(), kind=jnp.bfloat16):
    drawn = jax.random.normal(own_key, extent, jnp.float32) * spread
    if len(pieces) > 0:
        drawn = block_scale(own_key, extent, pieces, -0.22, 0.18) * drawn
    return jnp.clip(drawn, min=-most, max=most).astype(kind)


def setup_inputs(seed: int = 0) -> dict:
    splits = jax.random.split(jax.random.key(seed), 8)
    model_image = noise(splits[0], (TILES, TL, TM), (TILES * TL * TM) ** -0.5, 0.005859375, ((0, 2), (1, 4)))
    station_beams = noise(splits[1], (2, STATIONS, SG * SG), 1.0, 6.0, (), jnp.float32)
    subgrid_offsets = with_ends(jax.random.randint(splits[2], (N_CHAN, NSUB, 2), 0 - NG // 2, NG // 2 - SG + 1), jax.random.fold_in(splits[2], 1), 0 - NG // 2, (NG // 2 - SG + 1) - 1).astype(jnp.int32)
    subgrid_stations = draw_subgrid_stations(jax.random.fold_in(splits[7], 71), 0)
    visibility_uv = jnp.clip(2.0 + 28.0 * jax.random.uniform(splits[4], (2, NSUB, VROWS), jnp.float32) ** block_scale(splits[4], (2, NSUB, VROWS), ((1, 8), (2, 4)), -0.2, 0.2), 2.0, 30.0)
    observed = noise(splits[5], (2, NSUB // N_CHAN, N_CHAN, VROWS), 0.5, 3.0, ((1, 8), (2, 4)), jnp.float32)
    live_counts = with_ends(jax.random.randint(splits[6], (NSUB // N_CHAN, N_CHAN), 1, TIMES + 1), jax.random.fold_in(splits[6], 1), 1, TIMES).astype(jnp.int32)
    return dict(model_image=model_image, station_beams=station_beams, subgrid_offsets=subgrid_offsets, subgrid_stations=subgrid_stations, visibility_uv=visibility_uv, observed=observed, live_counts=live_counts)


two_pi = 6.283185307179586


def phase_pair(products, modulus):
    angle_turns = jnp.mod(products, modulus).astype(jnp.float32) * (two_pi / modulus)
    return jnp.cos(angle_turns), -jnp.sin(angle_turns)


def contract(pattern, left, right):
    return jnp.einsum(pattern, left.astype(jnp.float32), right.astype(jnp.float32), precision=lax.Precision.HIGHEST)


def tile_cuts(strip_rows, row_ids, offset_block, strip_half):
    block_size = offset_block.shape[0]
    columns = strip_rows.shape[1]
    pixel_idx = jnp.arange(SG, dtype=jnp.int32)
    col_pos = jnp.arange(columns, dtype=jnp.int32) - columns // 2
    v_index = offset_block[:, 1][:, None] + pixel_idx[None, :]
    ev_real, ev_imag = phase_pair(col_pos[:, None, None] * v_index[None, :, :], NG)
    phase_table = jnp.stack([ev_real, ev_imag], axis=1).reshape(columns, 2 * block_size * SG).astype(jnp.bfloat16)
    partial_q = jnp.dot(strip_rows, phase_table, preferred_element_type=jnp.float32).astype(jnp.bfloat16)
    partial_q = partial_q.reshape(strip_rows.shape[0], 2, block_size, SG)
    q_real = partial_q[:, 0]
    q_imag = partial_q[:, 1]
    u_index = offset_block[:, 0][:, None] + pixel_idx[None, :]
    row_pos = (row_ids - strip_half).astype(jnp.int32)
    eu_real, eu_imag = phase_pair(u_index[:, :, None] * row_pos[None, None, :], NG)
    eu_real = eu_real.astype(jnp.bfloat16)
    eu_imag = eu_imag.astype(jnp.bfloat16)
    cut_real = contract("jal,ljb->jab", eu_real, q_real) - contract("jal,ljb->jab", eu_imag, q_imag)
    cut_imag = contract("jal,ljb->jab", eu_real, q_imag) + contract("jal,ljb->jab", eu_imag, q_real)
    return jnp.stack([cut_real, cut_imag], axis=1).reshape(block_size, 2 * SG * SG)


def cuts_blocked(strip_rows, row_ids, offsets, strip_half):
    how_many = offsets.shape[0]
    block_size = math.gcd(how_many, 32)
    grouped = offsets.reshape(how_many // block_size, block_size, 2)
    stacked = lax.map(lambda offset_block: tile_cuts(strip_rows, row_ids, offset_block, strip_half), grouped)
    return stacked.reshape(how_many, 2 * SG * SG)


def predict(cut_rows, pair_ids, station_beams, uv_block):
    how_many = cut_rows.shape[0]
    cut_grid = cut_rows.reshape(how_many, 2, SG, SG)
    pixel_idx = jnp.arange(SG, dtype=jnp.int32)
    w_real, w_neg = phase_pair(pixel_idx[:, None] * pixel_idx[None, :], SG)
    w_imag = -w_neg
    c_real = cut_grid[:, 0]
    c_imag = cut_grid[:, 1]
    half_real = contract("xa,jab->jxb", w_real, c_real) - contract("xa,jab->jxb", w_imag, c_imag)
    half_imag = contract("xa,jab->jxb", w_real, c_imag) + contract("xa,jab->jxb", w_imag, c_real)
    sub_real = (contract("jxb,yb->jxy", half_real, w_real) - contract("jxb,yb->jxy", half_imag, w_imag)) / (SG * SG)
    sub_imag = (contract("jxb,yb->jxy", half_real, w_imag) + contract("jxb,yb->jxy", half_imag, w_real)) / (SG * SG)
    pixel_pos = pixel_idx.astype(jnp.float32)
    taper_line = 1.0 - ((2.0 * pixel_pos - (SG - 1)) / SG) ** 2
    taper_grid = (taper_line[:, None] * taper_line[None, :]).reshape(SG * SG)
    beam_first = station_beams[:, pair_ids[:, 0]]
    beam_second = station_beams[:, pair_ids[:, 1]]
    gain_real = (beam_first[0] * beam_second[0] + beam_first[1] * beam_second[1]) * taper_grid
    gain_imag = (beam_first[1] * beam_second[0] - beam_first[0] * beam_second[1]) * taper_grid
    flat_real = sub_real.reshape(how_many, SG * SG)
    flat_imag = sub_imag.reshape(how_many, SG * SG)
    weighted_real = (flat_real * gain_real - flat_imag * gain_imag).reshape(how_many, SG, SG)
    weighted_imag = (flat_real * gain_imag + flat_imag * gain_real).reshape(how_many, SG, SG)
    u_angle = uv_block[0][:, :, None] * pixel_pos[None, None, :] * (two_pi / SG)
    v_angle = uv_block[1][:, :, None] * pixel_pos[None, None, :] * (two_pi / SG)
    eu_real = jnp.cos(u_angle)
    eu_imag = -jnp.sin(u_angle)
    ev_real = jnp.cos(v_angle)
    ev_imag = -jnp.sin(v_angle)
    inner_real = contract("jxy,jky->jxk", weighted_real, ev_real) - contract("jxy,jky->jxk", weighted_imag, ev_imag)
    inner_imag = contract("jxy,jky->jxk", weighted_real, ev_imag) + contract("jxy,jky->jxk", weighted_imag, ev_real)
    vis_real = contract("jkx,jxk->jk", eu_real, inner_real) - contract("jkx,jxk->jk", eu_imag, inner_imag)
    vis_imag = contract("jkx,jxk->jk", eu_real, inner_imag) + contract("jkx,jxk->jk", eu_imag, inner_real)
    return jnp.stack([vis_real, vis_imag], axis=0)


def reference(model_image, station_beams, subgrid_offsets, subgrid_stations, visibility_uv, observed, live_counts):
    strip_rows = model_image.reshape(TILES * TL, TM)
    row_ids = jnp.arange(TILES * TL, dtype=jnp.int32)
    strip_half = TILES * TL // 2
    vis_width = CHAN_GRP * TIMES
    predicted_parts = []
    for channel_group in range(N_CHAN):
        cut_rows = cuts_blocked(strip_rows, row_ids, subgrid_offsets[channel_group], strip_half)
        uv_block = visibility_uv[:, :, channel_group * vis_width:(channel_group + 1) * vis_width]
        predicted_parts.append(predict(cut_rows, subgrid_stations, station_beams, uv_block))
    predicted = jnp.concatenate(predicted_parts, axis=2).reshape(2, NSUB // N_CHAN, N_CHAN, VROWS)
    time_step = jnp.mod(jnp.arange(VROWS, dtype=jnp.int32), TIMES)
    live_mask = time_step[None, None, :] < live_counts[:, :, None]
    return jnp.where(live_mask[None], observed - predicted, 0.0)
```

```python
import functools
import math

import jax
import jax.numpy as jnp
from jax import lax
from jax.experimental import pallas as pl
from jax.experimental.pallas import tpu as pltpu
from jax.sharding import PartitionSpec as P

SG = 32
NG = 8192
TIMES = 8
TILE_DEV = 4
TL = 64
SUB_TILE = 16
PACK = 4

MESH = pl.DeviceIdType.MESH
two_pi = 6.283185307179586


def phase_pair(products, modulus):
    angle_turns = jnp.mod(products, modulus).astype(jnp.float32) * (two_pi / modulus)
    return (jnp.cos(angle_turns), -jnp.sin(angle_turns))


def octant_polys(theta):
    z = theta * theta
    s = theta + theta * z * (
        -1.6666654611e-1 + z * (8.3321608736e-3 + z * -1.9515295891e-4)
    )
    c = 1.0 - 0.5 * z + z * z * (
        4.166664568298827e-2 + z * (-1.388731625493765e-3 + z * 2.443315711809948e-5)
    )
    return s, c


def turn_quadrant(quadrant, s, c):
    odd = (quadrant & 1) == 1
    cos_part = jnp.where(odd, s, c)
    sin_part = jnp.where(odd, c, s)
    cos_part = jnp.where(((quadrant + 1) & 2) == 2, -cos_part, cos_part)
    sin_part = jnp.where((quadrant & 2) == 2, sin_part, -sin_part)
    return cos_part, sin_part


def unit_phase(products):
    k = products & (NG - 1)
    quadrant = (k + NG // 8) >> (NG.bit_length() - 3)
    theta = (k - quadrant * (NG // 4)).astype(jnp.float32) * (two_pi / NG)
    s, c = octant_polys(theta)
    return turn_quadrant(quadrant, s, c)


def cmul(ar, ai, br, bi):
    return ar * br - ai * bi, ar * bi + ai * br


def dot_nt(a, b):
    return lax.dot_general(a, b, (((1,), (1,)), ((), ())), preferred_element_type=jnp.float32)


def remote(src, dst, send, recv, where):
    return pltpu.make_async_remote_copy(
        src_ref=src, dst_ref=dst, send_sem=send, recv_sem=recv, device_id=where, device_id_type=MESH
    )


def cuts_kernel(
    n_stn, n_chan, n_tile,
    x_ref, off_ref, out_ref,
    full, ar, ai, br, bi, cr, ci, dr, di, tab, eu, cuts, inbox,
    z_send, y_send, m_send, recv, cut_send, cut_recv,
):
    stn, chan, tile = lax.axis_index("stn"), lax.axis_index("chan"), lax.axis_index("tile")
    tiles, piece_rows, columns = x_ref.shape
    quarter = columns // n_chan
    rows = n_stn * tiles * piece_rows
    group = SUB_TILE * n_tile
    strip_half = TILE_DEV * n_tile * TL // 2
    mate, across = chan ^ 1, chan ^ 2
    hops = [1, n_stn - 1] + list(range(2, n_stn - 1))
    sources = [lax.rem(stn + d, n_stn) for d in hops]

    barrier = pltpu.get_barrier_semaphore()
    partners = [{"stn": s} for s in sources] + [{"chan": mate}, {"chan": across}]
    partners += [{"tile": lax.rem(tile + d, n_tile)} for d in range(1, n_tile)]
    for where in partners:
        pl.semaphore_signal(barrier, inc=1, device_id=where, device_id_type=MESH)
    pl.semaphore_wait(barrier, len(partners))

    own = x_ref.at[:, :, pl.ds(pl.multiple_of(chan * quarter, quarter), quarter)]
    z_copies = [
        remote(own, full.at[chan, stn], z_send.at[n], recv.at[chan, stn], {"stn": s})
        for n, s in enumerate(sources)
    ]
    for copy in z_copies:
        copy.start()
    for c in range(n_chan):
        full[c, stn] = x_ref[:, :, c * quarter:(c + 1) * quarter]

    first = pl.multiple_of(stn * group, group)
    col_pos = lax.broadcasted_iota(jnp.int32, (8, columns), 1) - columns // 2
    lane = lax.broadcasted_iota(jnp.int32, (8, rows), 1)
    shard = tiles * piece_rows
    row_s = lax.div(lane, shard)
    row_t = lax.div(lax.rem(lane, shard), piece_rows)
    row_pos = (tile * TILE_DEV + row_t) * TL + row_s * piece_rows + lax.rem(lane, piece_rows) - strip_half
    for step in range(SG // 8):
        part = slice(8 * step, 8 * step + 8)
        pixel = lax.broadcasted_iota(jnp.int32, (8, 1), 0) + 8 * step
        br[part], bi[part] = unit_phase(pixel * col_pos)
        dr[part], di[part] = unit_phase(pixel * row_pos)

    @pl.loop(0, group // 8)
    def _(step):
        at = pl.multiple_of(step * 8, 8)
        corners = off_ref[pl.ds(first + at, 8), :]
        ar[pl.ds(at, 8)], ai[pl.ds(at, 8)] = unit_phase(corners[:, 1:2] * col_pos)
        cr[pl.ds(at, 8)], ci[pl.ds(at, 8)] = unit_phase(corners[:, 0:1] * row_pos)

    @pl.loop(0, group // PACK)
    def _(pack):
        base = pl.multiple_of(pack * 2 * PACK * SG, 2 * PACK * SG)
        for n in range(PACK):
            j = pack * PACK + n
            real, imag = cmul(ar[pl.ds(j, 1)], ai[pl.ds(j, 1)], br[...], bi[...])
            tab[pl.ds(base + n * SG, SG)] = real.astype(jnp.bfloat16)
            tab[pl.ds(base + (PACK + n) * SG, SG)] = imag.astype(jnp.bfloat16)
            real, imag = cmul(cr[pl.ds(j, 1)], ci[pl.ds(j, 1)], dr[...], di[...])
            real, imag = real.astype(jnp.bfloat16), imag.astype(jnp.bfloat16)
            eu[pl.ds(base + n * SG, SG), :rows] = real
            eu[pl.ds(base + n * SG, SG), rows:] = -imag
            eu[pl.ds(base + (PACK + n) * SG, SG), :rows] = imag
            eu[pl.ds(base + (PACK + n) * SG, SG), rows:] = real

    onward = []
    for n, s in enumerate(sources):
        piece = full.at[chan, s]
        remote(own, piece, z_send.at[n], recv.at[chan, s], {"stn": s}).wait_recv()
        for sems, slot, where in ((y_send, n, across), (m_send, n, mate)):
            copy = remote(piece, piece, sems.at[slot], recv.at[chan, s], {"chan": where})
            copy.start()
            onward.append(copy)
    for n, s in enumerate(sources):
        piece = full.at[across, s]
        remote(piece, piece, y_send.at[n], recv.at[across, s], {"chan": across}).wait_recv()
        copy = remote(piece, piece, m_send.at[len(sources) + n], recv.at[across, s], {"chan": mate})
        copy.start()
        onward.append(copy)
    for n, s in enumerate(sources):
        for c in (mate, mate ^ 2):
            piece = full.at[c, s]
            remote(piece, piece, y_send.at[n], recv.at[c, s], {"chan": mate}).wait_recv()
    for copy in z_copies + onward:
        copy.wait_send()

    lane_pack = lax.broadcasted_iota(jnp.int32, (SG, PACK * SG), 1) >> (SG.bit_length() - 1)

    def own_block(half):
        picked = half[:SG]
        for n in range(1, PACK):
            picked = jnp.where(lane_pack == n, half[n * SG:(n + 1) * SG], picked)
        return picked

    packs = SUB_TILE // PACK
    both = 2 * PACK * SG
    per_step = 2
    sent = []
    for d in range(1, n_tile + 1):
        peer = lax.rem(tile + d, n_tile)

        @pl.loop(0, packs // per_step)
        def _(step):
            pack = peer * packs + step * per_step
            at = pl.multiple_of(pack * both, both)
            q = dot_nt(tab[pl.ds(at, per_step * both), :quarter], full[0].reshape(rows, quarter))
            for c in range(1, n_chan):
                q += dot_nt(
                    tab[pl.ds(at, per_step * both), c * quarter:(c + 1) * quarter],
                    full[c].reshape(rows, quarter),
                )
            q = q.astype(jnp.bfloat16)
            for k in range(per_step):
                top = k * both
                q_k = jnp.concatenate(
                    [q[top:top + both // 2], q[top + both // 2:top + both]], axis=1
                )
                cut = dot_nt(eu[pl.ds(at + top, both)], q_k)
                cuts[pack + k, :SG] = own_block(cut[:both // 2])
                cuts[pack + k, SG:] = own_block(cut[both // 2:])

        if d < n_tile:
            copy = remote(
                cuts.at[pl.ds(peer * packs, packs)], inbox.at[d - 1],
                cut_send.at[d - 1], cut_recv.at[d - 1], {"tile": peer},
            )
            copy.start()
            sent.append(copy)
    total = cuts[pl.ds(tile * packs, packs)]
    for d, copy in enumerate(sent):
        copy.wait()
        total += inbox[d]
    out_ref[...] = total


def own_cuts_call(model_image, offsets):
    n_stn, n_chan, n_tile = (lax.axis_size(a) for a in ("stn", "chan", "tile"))
    tiles, piece_rows, columns = model_image.shape
    rows = n_stn * tiles * piece_rows
    group = SUB_TILE * n_tile
    packs = SUB_TILE // PACK
    f32, bf16 = jnp.float32, jnp.bfloat16
    vmem = pl.BlockSpec(memory_space=pltpu.VMEM)
    dma = pltpu.SemaphoreType.DMA
    return pl.pallas_call(
        functools.partial(cuts_kernel, n_stn, n_chan, n_tile),
        out_shape=jax.ShapeDtypeStruct((packs, 2 * SG, PACK * SG), f32),
        in_specs=[vmem, vmem],
        out_specs=vmem,
        scratch_shapes=[
            pltpu.VMEM((n_chan, n_stn, tiles, piece_rows, columns // n_chan), bf16),
            pltpu.VMEM((group, columns), f32),
            pltpu.VMEM((group, columns), f32),
            pltpu.VMEM((SG, columns), f32),
            pltpu.VMEM((SG, columns), f32),
            pltpu.VMEM((group, rows), f32),
            pltpu.VMEM((group, rows), f32),
            pltpu.VMEM((SG, rows), f32),
            pltpu.VMEM((SG, rows), f32),
            pltpu.VMEM((group * 2 * SG, columns), bf16),
            pltpu.VMEM((group * 2 * SG, 2 * rows), bf16),
            pltpu.VMEM((group // PACK, 2 * SG, PACK * SG), f32),
            pltpu.VMEM((max(n_tile - 1, 1), packs, 2 * SG, PACK * SG), f32),
            dma((n_stn - 1,)),
            dma((n_stn - 1,)),
            dma((2 * (n_stn - 1),)),
            dma((n_chan, n_stn)),
            dma((max(n_tile - 1, 1),)),
            dma((max(n_tile - 1, 1),)),
        ],
        compiler_params=pltpu.CompilerParams(
            collective_id=0, has_side_effects=True, vmem_limit_bytes=60 * 1024 * 1024
        ),
    )(model_image, offsets)


def exact_mix(pattern, left, right):
    return jnp.einsum(pattern, left, right, precision=lax.Precision.HIGHEST)


def predict(cut_rows, pair_ids, station_beams, uv_block):
    how_many = cut_rows.shape[0]
    cut_grid = cut_rows.reshape(how_many, 2, SG, SG)
    pixel_idx = jnp.arange(SG, dtype=jnp.int32)
    w_real, w_neg = phase_pair(pixel_idx[:, None] * pixel_idx[None, :], SG)
    w_imag = -w_neg
    c_real = cut_grid[:, 0]
    c_imag = cut_grid[:, 1]
    half_real = exact_mix("xa,jab->jxb", w_real, c_real) - exact_mix("xa,jab->jxb", w_imag, c_imag)
    half_imag = exact_mix("xa,jab->jxb", w_real, c_imag) + exact_mix("xa,jab->jxb", w_imag, c_real)
    sub_real = (
        exact_mix("jxb,yb->jxy", half_real, w_real) - exact_mix("jxb,yb->jxy", half_imag, w_imag)
    ) / (SG * SG)
    sub_imag = (
        exact_mix("jxb,yb->jxy", half_real, w_imag) + exact_mix("jxb,yb->jxy", half_imag, w_real)
    ) / (SG * SG)
    pixel_pos = pixel_idx.astype(jnp.float32)
    taper_line = 1.0 - ((2.0 * pixel_pos - (SG - 1)) / SG) ** 2
    taper_grid = (taper_line[:, None] * taper_line[None, :]).reshape(SG * SG)
    beam_first = station_beams[:, pair_ids[:, 0]]
    beam_second = station_beams[:, pair_ids[:, 1]]
    gain_real = (beam_first[0] * beam_second[0] + beam_first[1] * beam_second[1]) * taper_grid
    gain_imag = (beam_first[1] * beam_second[0] - beam_first[0] * beam_second[1]) * taper_grid
    flat_real = sub_real.reshape(how_many, SG * SG)
    flat_imag = sub_imag.reshape(how_many, SG * SG)
    weighted_real = (flat_real * gain_real - flat_imag * gain_imag).reshape(how_many, SG, SG)
    weighted_imag = (flat_real * gain_imag + flat_imag * gain_real).reshape(how_many, SG, SG)
    u_angle = uv_block[0][:, :, None] * pixel_pos[None, None, :] * (two_pi / SG)
    v_angle = uv_block[1][:, :, None] * pixel_pos[None, None, :] * (two_pi / SG)
    eu_real = jnp.cos(u_angle)
    eu_imag = -jnp.sin(u_angle)
    ev_real = jnp.cos(v_angle)
    ev_imag = -jnp.sin(v_angle)
    inner_real = exact_mix("jxy,jky->jxk", weighted_real, ev_real) - exact_mix(
        "jxy,jky->jxk", weighted_imag, ev_imag
    )
    inner_imag = exact_mix("jxy,jky->jxk", weighted_real, ev_imag) + exact_mix(
        "jxy,jky->jxk", weighted_imag, ev_real
    )
    vis_real = exact_mix("jkx,jxk->jk", eu_real, inner_real) - exact_mix(
        "jkx,jxk->jk", eu_imag, inner_imag
    )
    vis_imag = exact_mix("jkx,jxk->jk", eu_real, inner_imag) + exact_mix(
        "jkx,jxk->jk", eu_imag, inner_real
    )
    return jnp.stack([vis_real, vis_imag], axis=0)


def on_device(
    model_image,
    station_beams,
    subgrid_offsets,
    subgrid_stations,
    visibility_uv,
    observed,
    live_counts,
):
    packed = own_cuts_call(model_image, subgrid_offsets[0])
    own_cuts = packed.reshape(SUB_TILE // PACK, 2, SG, PACK, SG).transpose(0, 3, 1, 2, 4)
    own_cuts = own_cuts.reshape(SUB_TILE, 2 * SG * SG)
    predicted = predict(own_cuts, subgrid_stations, station_beams, visibility_uv)
    chan_count = lax.axis_size("chan")
    outgoing = predicted.reshape(2, SUB_TILE // chan_count, chan_count, predicted.shape[2])
    regrouped = lax.all_to_all(outgoing, "chan", split_axis=2, concat_axis=3, tiled=True)
    total_rows = regrouped.shape[3]
    time_step = jnp.mod(jnp.arange(total_rows, dtype=jnp.int32), TIMES)
    live_mask = time_step[None, None, :] < live_counts[:, :, None]
    return jnp.where(live_mask[None], observed - regrouped, 0.0)


def solution(mesh):
    return jax.shard_map(
        on_device,
        mesh=mesh,
        in_specs=(
            P("tile", "stn", None),
            P(),
            P("chan", None, None),
            P(("stn", "tile"), None),
            P(None, ("stn", "tile"), "chan"),
            P(None, ("stn", "tile"), "chan", None),
            P(("stn", "tile"), "chan"),
        ),
        out_specs=P(None, ("stn", "tile"), "chan", None),
        check_vma=False,
    )
```

```python
import functools

import jax
import jax.numpy as jnp
from jax import lax
from jax.experimental import pallas as pl
from jax.experimental.pallas import tpu as pltpu
from jax.sharding import PartitionSpec as P

SG = 32
NG = 8192
TIMES = 8
TILE_DEV = 4
TL = 64
SUB_TILE = 16
PACK = 4

MESH = pl.DeviceIdType.MESH
two_pi = 6.283185307179586


def octant_polys(theta):
    z = theta * theta
    s = theta + theta * z * (
        -1.6666654611e-1 + z * (8.3321608736e-3 + z * -1.9515295891e-4)
    )
    c = 1.0 - 0.5 * z + z * z * (
        4.166664568298827e-2 + z * (-1.388731625493765e-3 + z * 2.443315711809948e-5)
    )
    return s, c


def turn_quadrant(quadrant, s, c):
    odd = (quadrant & 1) == 1
    cos_part = jnp.where(odd, s, c)
    sin_part = jnp.where(odd, c, s)
    cos_part = jnp.where(((quadrant + 1) & 2) == 2, -cos_part, cos_part)
    sin_part = jnp.where((quadrant & 2) == 2, sin_part, -sin_part)
    return cos_part, sin_part


def unit_phase(products):
    k = products & (NG - 1)
    quadrant = (k + NG // 8) >> (NG.bit_length() - 3)
    theta = (k - quadrant * (NG // 4)).astype(jnp.float32) * (two_pi / NG)
    s, c = octant_polys(theta)
    return turn_quadrant(quadrant, s, c)


def turn_fraction(turns):
    quadrant = jnp.floor(turns * (4.0 / SG) + 0.5)
    theta = (turns - quadrant * (SG / 4.0)) * (two_pi / SG)
    s, c = octant_polys(theta)
    return turn_quadrant(quadrant.astype(jnp.int32), s, c)


def dft_entries(out_part, out_pixel, in_part, in_pixel):
    turns = out_pixel * in_pixel + (SG // 4) * (in_part - out_part)
    return unit_phase(turns * (NG // SG))[0]


def split(x):
    high = x.astype(jnp.bfloat16)
    return high, (x - high.astype(jnp.float32)).astype(jnp.bfloat16)


def dot_nn(a, b):
    return jnp.dot(a, b, preferred_element_type=jnp.float32)


def iota(shape, axis):
    return lax.broadcasted_iota(jnp.int32, shape, axis)


def cmul(ar, ai, br, bi):
    return ar * br - ai * bi, ar * bi + ai * br


def dot_nt(a, b):
    return lax.dot_general(a, b, (((1,), (1,)), ((), ())), preferred_element_type=jnp.float32)


def remote(src, dst, send, recv, where):
    return pltpu.make_async_remote_copy(
        src_ref=src, dst_ref=dst, send_sem=send, recv_sem=recv, device_id=where, device_id_type=MESH
    )


def prediction_tables(pair_ref, beam_ref, uv_ref, beams, gain, dft_x, dft_y, ev, uu):
    log_sg, half = SG.bit_length() - 1, PACK * SG
    rows_at = SG // PACK
    packs = SUB_TILE // PACK

    shape = (2 * SG, 6 * SG)
    row, col = iota(shape, 0), iota(shape, 1)
    line = row & (SG - 1)
    x = PACK * (line & (rows_at - 1)) + line // rows_at
    entries = dft_entries(row >> log_sg, x, (col >> log_sg) & 1, col & (SG - 1))
    high, low = split(entries)
    dft_x[...] = jnp.where(col >= 4 * SG, low.astype(jnp.float32), high.astype(jnp.float32)).astype(
        jnp.bfloat16
    )

    shape = (half, 2 * half)
    for part in range(2):
        row, col = iota(shape, 0), iota(shape, 1)
        out_part = (col >= half).astype(jnp.int32)
        entries = dft_entries(out_part, col & (SG - 1), part, row & (SG - 1))
        same = (row >> log_sg) == ((col >> log_sg) & (PACK - 1))
        high, low = split(jnp.where(same, entries * (1.0 / (SG * SG)), 0.0))
        dft_y[0, part * half:(part + 1) * half] = high
        dft_y[1, part * half:(part + 1) * half] = low

    @pl.loop(0, SUB_TILE)
    def _(j):
        for side in range(2):
            station = pair_ref[side, j]
            for part in range(2):
                flat = beam_ref[part, pl.ds(station, 1)]
                for c in range(rows_at):
                    beams[side, part, j, c:c + 1] = flat[:, c * half:(c + 1) * half]

    shape = (rows_at, half)
    lane = iota(shape, 1)
    lane_pack = lane >> log_sg

    def taper(pixel):
        return 1.0 - ((2.0 * pixel.astype(jnp.float32) - (SG - 1)) / SG) ** 2

    tapers = taper(PACK * iota(shape, 0) + lane_pack) * taper(lane & (SG - 1))
    pixel = iota((SG, 1), 0)
    y_pixel = pixel.astype(jnp.float32)
    x_pixel = (PACK * (pixel & (rows_at - 1)) + pixel // rows_at).astype(jnp.float32)

    @pl.loop(0, packs)
    def _(p):
        gains = []
        for n in range(PACK):
            j = p * PACK + n
            one_r, one_i = beams[0, 0, j], beams[0, 1, j]
            two_r, two_i = beams[1, 0, j], beams[1, 1, j]
            gains.append(
                ((one_r * two_r + one_i * two_i) * tapers, (one_i * two_r - one_r * two_i) * tapers)
            )
            at = slice(n * SG, (n + 1) * SG)
            real, imag = turn_fraction(uv_ref[1, pl.ds(j, 1)] * y_pixel)
            for k, (er, ei) in enumerate(zip(split(real), split(imag))):
                ev[k, p, n * SG:(n + 1) * SG, :half] = er
                ev[k, p, n * SG:(n + 1) * SG, half:] = ei
                ev[k, p, half + n * SG:half + (n + 1) * SG, :half] = -ei
                ev[k, p, half + n * SG:half + (n + 1) * SG, half:] = er
            uu[0, p, at], uu[1, p, at] = turn_fraction(uv_ref[0, pl.ds(j, 1)] * x_pixel)
        for part in range(2):
            for q in range(PACK):
                picked = None
                for n in range(PACK):
                    shift = (n - q) * SG % half
                    moved = gains[n][part]
                    moved = pltpu.roll(moved, shift, axis=1) if shift else moved
                    picked = moved if n == 0 else jnp.where(lane_pack == n, moved, picked)
                gain[part, p, q * rows_at:(q + 1) * rows_at] = picked


def predict_kernel(
    n_stn, n_chan, n_tile,
    x_ref, off_ref, pair_ref, beam_ref, uv_ref, out_ref,
    full, ar, ai, br, bi, cr, ci, dr, di, tab, eu, cuts, inbox,
    beams, gain, dft_x, dft_y, ev, uu, outbox, box,
    z_send, y_send, m_send, recv, cut_send, cut_recv, vis_send, vis_recv,
):
    stn, chan, tile = lax.axis_index("stn"), lax.axis_index("chan"), lax.axis_index("tile")
    tiles, piece_rows, columns = x_ref.shape
    quarter = columns // n_chan
    rows = n_stn * tiles * piece_rows
    group = SUB_TILE * n_tile
    strip_half = TILE_DEV * n_tile * TL // 2
    mate, across = chan ^ 1, chan ^ 2
    hops = [1, n_stn - 1] + list(range(2, n_stn - 1))
    sources = [lax.rem(stn + d, n_stn) for d in hops]

    barrier = pltpu.get_barrier_semaphore()
    partners = [{"stn": s} for s in sources] + [{"chan": lax.rem(chan + d, n_chan)} for d in range(1, n_chan)]
    partners += [{"tile": lax.rem(tile + d, n_tile)} for d in range(1, n_tile)]
    for where in partners:
        pl.semaphore_signal(barrier, inc=1, device_id=where, device_id_type=MESH)
    pl.semaphore_wait(barrier, len(partners))

    own = x_ref.at[:, :, pl.ds(pl.multiple_of(chan * quarter, quarter), quarter)]
    z_copies = [
        remote(own, full.at[chan, stn], z_send.at[n], recv.at[chan, stn], {"stn": s})
        for n, s in enumerate(sources)
    ]
    for copy in z_copies:
        copy.start()
    for c in range(n_chan):
        full[c, stn] = x_ref[:, :, c * quarter:(c + 1) * quarter]

    first = pl.multiple_of(stn * group, group)
    col_pos = lax.broadcasted_iota(jnp.int32, (8, columns), 1) - columns // 2
    lane = lax.broadcasted_iota(jnp.int32, (8, rows), 1)
    shard = tiles * piece_rows
    row_s = lax.div(lane, shard)
    row_t = lax.div(lax.rem(lane, shard), piece_rows)
    row_pos = (tile * TILE_DEV + row_t) * TL + row_s * piece_rows + lax.rem(lane, piece_rows) - strip_half
    for step in range(SG // 8):
        part = slice(8 * step, 8 * step + 8)
        pixel = lax.broadcasted_iota(jnp.int32, (8, 1), 0) + 8 * step
        br[part], bi[part] = unit_phase(pixel * col_pos)
        dr[part], di[part] = unit_phase(pixel * row_pos)

    @pl.loop(0, group // 8)
    def _(step):
        at = pl.multiple_of(step * 8, 8)
        u_first = jnp.zeros((8, 1), jnp.int32)
        v_first = u_first
        for n in range(8):
            here = iota((8, 1), 0) == n
            u_first = jnp.where(here, off_ref[0, first + at + n], u_first)
            v_first = jnp.where(here, off_ref[1, first + at + n], v_first)
        ar[pl.ds(at, 8)], ai[pl.ds(at, 8)] = unit_phase(v_first * col_pos)
        cr[pl.ds(at, 8)], ci[pl.ds(at, 8)] = unit_phase(u_first * row_pos)

    @pl.loop(0, group // PACK)
    def _(pack):
        base = pl.multiple_of(pack * 2 * PACK * SG, 2 * PACK * SG)
        for n in range(PACK):
            j = pack * PACK + n
            real, imag = cmul(ar[pl.ds(j, 1)], ai[pl.ds(j, 1)], br[...], bi[...])
            tab[pl.ds(base + n * SG, SG)] = real.astype(jnp.bfloat16)
            tab[pl.ds(base + (PACK + n) * SG, SG)] = imag.astype(jnp.bfloat16)
            real, imag = cmul(cr[pl.ds(j, 1)], ci[pl.ds(j, 1)], dr[...], di[...])
            real, imag = real.astype(jnp.bfloat16), imag.astype(jnp.bfloat16)
            eu[pl.ds(base + n * SG, SG), :rows] = real
            eu[pl.ds(base + n * SG, SG), rows:] = -imag
            eu[pl.ds(base + (PACK + n) * SG, SG), :rows] = imag
            eu[pl.ds(base + (PACK + n) * SG, SG), rows:] = real

    onward = []
    for n, s in enumerate(sources):
        piece = full.at[chan, s]
        remote(own, piece, z_send.at[n], recv.at[chan, s], {"stn": s}).wait_recv()
        for sems, slot, where in ((y_send, n, across), (m_send, n, mate)):
            copy = remote(piece, piece, sems.at[slot], recv.at[chan, s], {"chan": where})
            copy.start()
            onward.append(copy)
    prediction_tables(pair_ref, beam_ref, uv_ref, beams, gain, dft_x, dft_y, ev, uu)
    for n, s in enumerate(sources):
        piece = full.at[across, s]
        remote(piece, piece, y_send.at[n], recv.at[across, s], {"chan": across}).wait_recv()
        copy = remote(piece, piece, m_send.at[len(sources) + n], recv.at[across, s], {"chan": mate})
        copy.start()
        onward.append(copy)
    for n, s in enumerate(sources):
        for c in (mate, mate ^ 2):
            piece = full.at[c, s]
            remote(piece, piece, y_send.at[n], recv.at[c, s], {"chan": mate}).wait_recv()
    for copy in z_copies + onward:
        copy.wait_send()

    lane_pack = lax.broadcasted_iota(jnp.int32, (SG, PACK * SG), 1) >> (SG.bit_length() - 1)

    def own_block(half):
        picked = half[:SG]
        for n in range(1, PACK):
            picked = jnp.where(lane_pack == n, half[n * SG:(n + 1) * SG], picked)
        return picked

    packs = SUB_TILE // PACK
    both = 2 * PACK * SG
    half = PACK * SG
    per_step = 2
    sent = []
    for d in range(1, n_tile + 1):
        peer = lax.rem(tile + d, n_tile)

        @pl.loop(0, packs // per_step)
        def _(step):
            pack = peer * packs + step * per_step
            at = pl.multiple_of(pack * both, both)
            q = dot_nt(tab[pl.ds(at, per_step * both), :quarter], full[0].reshape(rows, quarter))
            for c in range(1, n_chan):
                q += dot_nt(
                    tab[pl.ds(at, per_step * both), c * quarter:(c + 1) * quarter],
                    full[c].reshape(rows, quarter),
                )
            q = q.astype(jnp.bfloat16)
            for k in range(per_step):
                top = k * both
                q_k = jnp.concatenate(
                    [q[top:top + both // 2], q[top + both // 2:top + both]], axis=1
                )
                cut = dot_nt(eu[pl.ds(at + top, both)], q_k)
                cuts[pack + k, :SG] = own_block(cut[:both // 2])
                cuts[pack + k, SG:] = own_block(cut[both // 2:])

        if d < n_tile:
            copy = remote(
                cuts.at[pl.ds(peer * packs, packs)], inbox.at[d - 1],
                cut_send.at[d - 1], cut_recv.at[d - 1], {"tile": peer},
            )
            copy.start()
            sent.append(copy)
    total = cuts[pl.ds(tile * packs, packs)]
    for d, copy in enumerate(sent):
        copy.wait()
        total += inbox[d]
    lines = []
    for p in range(packs):
        high, low = split(total[p])
        z = dot_nn(dft_x[...], jnp.concatenate([high, low, high], axis=0))
        lines.append(jnp.concatenate([z[:SG], z[SG:]], axis=1))
    high, low = split(jnp.concatenate(lines, axis=0))
    sub = dot_nn(high, dft_y[0]) + dot_nn(low, dft_y[0]) + dot_nn(high, dft_y[1])
    lane_pair = (iota((SG, both), 1) >> (SG.bit_length() - 1)) & (PACK - 1)
    for p in range(packs):
        sub_p = sub[p * SG:(p + 1) * SG]
        real, imag = cmul(sub_p[:, :half], sub_p[:, half:], gain[0, p], gain[1, p])
        weighted = jnp.concatenate([real, imag], axis=1)
        apart = [jnp.where(lane_pair == n, weighted, 0.0) for n in range(PACK)]
        high, low = split(jnp.concatenate(apart, axis=0))
        inner = dot_nn(high, ev[0, p]) + dot_nn(low, ev[0, p]) + dot_nn(high, ev[1, p])
        real, imag = cmul(uu[0, p], uu[1, p], inner[:, :half], inner[:, half:])
        outbox[:, 0, p] = real.reshape(PACK, SG, half).sum(axis=1)
        outbox[:, 1, p] = imag.reshape(PACK, SG, half).sum(axis=1)

    sent = []
    for d in range(1, n_chan):
        to = lax.rem(chan + d, n_chan)
        copy = remote(
            outbox.at[to], box.at[chan], vis_send.at[d - 1], vis_recv.at[chan], {"chan": to}
        )
        copy.start()
        sent.append(copy)
    box[chan] = outbox[chan]
    for d in range(1, n_chan):
        source = lax.rem(chan + d, n_chan)
        remote(
            outbox.at[source], box.at[source], vis_send.at[d - 1], vis_recv.at[source],
            {"chan": source},
        ).wait_recv()
    for g in range(n_chan):
        out_ref[:, :, 0, g * half:(g + 1) * half] = box[g]
    for copy in sent:
        copy.wait_send()


def predict_call(model_image, offsets, pair_ids, station_beams, uv_block):
    n_stn, n_chan, n_tile = (lax.axis_size(a) for a in ("stn", "chan", "tile"))
    tiles, piece_rows, columns = model_image.shape
    rows = n_stn * tiles * piece_rows
    group = SUB_TILE * n_tile
    packs = SUB_TILE // PACK
    f32, bf16 = jnp.float32, jnp.bfloat16
    half = PACK * SG
    assert PACK == n_chan
    vmem = pl.BlockSpec(memory_space=pltpu.VMEM)
    smem = pl.BlockSpec(memory_space=pltpu.SMEM)
    dma = pltpu.SemaphoreType.DMA
    return pl.pallas_call(
        functools.partial(predict_kernel, n_stn, n_chan, n_tile),
        out_shape=jax.ShapeDtypeStruct((2, packs, 1, n_chan * half), f32),
        in_specs=[vmem, smem, smem, vmem, vmem],
        out_specs=vmem,
        scratch_shapes=[
            pltpu.VMEM((n_chan, n_stn, tiles, piece_rows, columns // n_chan), bf16),
            pltpu.VMEM((group, columns), f32),
            pltpu.VMEM((group, columns), f32),
            pltpu.VMEM((SG, columns), f32),
            pltpu.VMEM((SG, columns), f32),
            pltpu.VMEM((group, rows), f32),
            pltpu.VMEM((group, rows), f32),
            pltpu.VMEM((SG, rows), f32),
            pltpu.VMEM((SG, rows), f32),
            pltpu.VMEM((group * 2 * SG, columns), bf16),
            pltpu.VMEM((group * 2 * SG, 2 * rows), bf16),
            pltpu.VMEM((group // PACK, 2 * SG, PACK * SG), f32),
            pltpu.VMEM((max(n_tile - 1, 1), packs, 2 * SG, PACK * SG), f32),
            pltpu.VMEM((2, 2, SUB_TILE, SG // PACK, half), f32),
            pltpu.VMEM((2, packs, SG, half), f32),
            pltpu.VMEM((2 * SG, 6 * SG), bf16),
            pltpu.VMEM((2, 2 * half, 2 * half), bf16),
            pltpu.VMEM((2, packs, 2 * half, 2 * half), bf16),
            pltpu.VMEM((2, packs, half, half), f32),
            pltpu.VMEM((n_chan, 2, packs, half), f32),
            pltpu.VMEM((n_chan, 2, packs, half), f32),
            dma((n_stn - 1,)),
            dma((n_stn - 1,)),
            dma((2 * (n_stn - 1),)),
            dma((n_chan, n_stn)),
            dma((max(n_tile - 1, 1),)),
            dma((max(n_tile - 1, 1),)),
            dma((n_chan - 1,)),
            dma((n_chan,)),
        ],
        compiler_params=pltpu.CompilerParams(
            collective_id=0, has_side_effects=True, vmem_limit_bytes=60 * 1024 * 1024
        ),
    )(model_image, offsets.T, pair_ids.T, station_beams, uv_block)


def on_device(
    model_image,
    station_beams,
    subgrid_offsets,
    subgrid_stations,
    visibility_uv,
    observed,
    live_counts,
):
    regrouped = predict_call(
        model_image, subgrid_offsets[0], subgrid_stations, station_beams, visibility_uv
    )
    total_rows = regrouped.shape[3]
    time_step = jnp.mod(jnp.arange(total_rows, dtype=jnp.int32), TIMES)
    live_mask = time_step[None, None, :] < live_counts[:, :, None]
    return jnp.where(live_mask[None], observed - regrouped, 0.0)


def solution(mesh):
    return jax.shard_map(
        on_device,
        mesh=mesh,
        in_specs=(
            P("tile", "stn", None),
            P(),
            P("chan", None, None),
            P(("stn", "tile"), None),
            P(None, ("stn", "tile"), "chan"),
            P(None, ("stn", "tile"), "chan", None),
            P(("stn", "tile"), "chan"),
        ),
        out_specs=P(None, ("stn", "tile"), "chan", None),
        check_vma=False,
    )
```

```python
import functools

import jax
import jax.numpy as jnp
from jax import lax
from jax.experimental import pallas as pl
from jax.experimental.pallas import tpu as pltpu
from jax.sharding import PartitionSpec as P

SG = 32
NG = 8192
TIMES = 8
TILE_DEV = 4
TL = 64
SUB_TILE = 16
CUTS = 1
PACK = 4

MESH = pl.DeviceIdType.MESH
two_pi = 6.283185307179586


def octant_polys(theta):
    z = theta * theta
    s = theta + theta * z * (
        -1.6666654611e-1 + z * (8.3321608736e-3 + z * -1.9515295891e-4)
    )
    c = 1.0 - 0.5 * z + z * z * (
        4.166664568298827e-2 + z * (-1.388731625493765e-3 + z * 2.443315711809948e-5)
    )
    return s, c


def turn_quadrant(quadrant, s, c):
    odd = (quadrant & 1) == 1
    cos_part = jnp.where(odd, s, c)
    sin_part = jnp.where(odd, c, s)
    cos_part = jnp.where(((quadrant + 1) & 2) == 2, -cos_part, cos_part)
    sin_part = jnp.where((quadrant & 2) == 2, sin_part, -sin_part)
    return cos_part, sin_part


def unit_phase(products):
    k = products & (NG - 1)
    quadrant = (k + NG // 8) >> (NG.bit_length() - 3)
    theta = (k - quadrant * (NG // 4)).astype(jnp.float32) * (two_pi / NG)
    s, c = octant_polys(theta)
    return turn_quadrant(quadrant, s, c)


def turn_fraction(turns):
    quadrant = jnp.floor(turns * (4.0 / SG) + 0.5)
    theta = (turns - quadrant * (SG / 4.0)) * (two_pi / SG)
    s, c = octant_polys(theta)
    return turn_quadrant(quadrant.astype(jnp.int32), s, c)


def dft_entries(out_part, out_pixel, in_part, in_pixel):
    turns = out_pixel * in_pixel + (SG // 4) * (in_part - out_part)
    return unit_phase(turns * (NG // SG))[0]


def split(x):
    high = x.astype(jnp.bfloat16)
    return high, (x - high.astype(jnp.float32)).astype(jnp.bfloat16)


def dot_nn(a, b):
    return jnp.dot(a, b, preferred_element_type=jnp.float32)


def iota(shape, axis):
    return lax.broadcasted_iota(jnp.int32, shape, axis)


def cmul(ar, ai, br, bi):
    return ar * br - ai * bi, ar * bi + ai * br


def dot_nt(a, b):
    return lax.dot_general(a, b, (((1,), (1,)), ((), ())), preferred_element_type=jnp.float32)


def remote(src, dst, send, recv, where):
    return pltpu.make_async_remote_copy(
        src_ref=src, dst_ref=dst, send_sem=send, recv_sem=recv, device_id=where, device_id_type=MESH
    )


def prediction_tables(pair_ref, beam_ref, uv_ref, beams, gain, dft_x, dft_y, ev, uu):
    log_sg, half = SG.bit_length() - 1, PACK * SG
    rows_at = SG // PACK
    packs = SUB_TILE // PACK

    shape = (2 * SG, 6 * SG)
    row, col = iota(shape, 0), iota(shape, 1)
    line = row & (SG - 1)
    x = PACK * (line & (rows_at - 1)) + line // rows_at
    entries = dft_entries(row >> log_sg, x, (col >> log_sg) & 1, col & (SG - 1))
    high, low = split(entries)
    dft_x[...] = jnp.where(col >= 4 * SG, low.astype(jnp.float32), high.astype(jnp.float32)).astype(
        jnp.bfloat16
    )

    shape = (half, 2 * half)
    for part in range(2):
        row, col = iota(shape, 0), iota(shape, 1)
        out_part = (col >= half).astype(jnp.int32)
        entries = dft_entries(out_part, col & (SG - 1), part, row & (SG - 1))
        same = (row >> log_sg) == ((col >> log_sg) & (PACK - 1))
        high, low = split(jnp.where(same, entries * (1.0 / (SG * SG)), 0.0))
        dft_y[0, part * half:(part + 1) * half] = high
        dft_y[1, part * half:(part + 1) * half] = low

    @pl.loop(0, SUB_TILE)
    def _(j):
        for side in range(2):
            station = pair_ref[side, j]
            for part in range(2):
                flat = beam_ref[part, pl.ds(station, 1)]
                for c in range(rows_at):
                    beams[side, part, j, c:c + 1] = flat[:, c * half:(c + 1) * half]

    shape = (rows_at, half)
    lane = iota(shape, 1)
    lane_pack = lane >> log_sg

    def taper(pixel):
        return 1.0 - ((2.0 * pixel.astype(jnp.float32) - (SG - 1)) / SG) ** 2

    tapers = taper(PACK * iota(shape, 0) + lane_pack) * taper(lane & (SG - 1))
    pixel = iota((SG, 1), 0)
    y_pixel = pixel.astype(jnp.float32)
    x_pixel = (PACK * (pixel & (rows_at - 1)) + pixel // rows_at).astype(jnp.float32)

    @pl.loop(0, packs)
    def _(p):
        gains = []
        for n in range(PACK):
            j = p * PACK + n
            one_r, one_i = beams[0, 0, j], beams[0, 1, j]
            two_r, two_i = beams[1, 0, j], beams[1, 1, j]
            gains.append(
                ((one_r * two_r + one_i * two_i) * tapers, (one_i * two_r - one_r * two_i) * tapers)
            )
            at = slice(n * SG, (n + 1) * SG)
            real, imag = turn_fraction(uv_ref[1, pl.ds(j, 1)] * y_pixel)
            for k, (er, ei) in enumerate(zip(split(real), split(imag))):
                ev[k, p, n * SG:(n + 1) * SG, :half] = er
                ev[k, p, n * SG:(n + 1) * SG, half:] = ei
                ev[k, p, half + n * SG:half + (n + 1) * SG, :half] = -ei
                ev[k, p, half + n * SG:half + (n + 1) * SG, half:] = er
            uu[0, p, at], uu[1, p, at] = turn_fraction(uv_ref[0, pl.ds(j, 1)] * x_pixel)
        for part in range(2):
            for q in range(PACK):
                picked = None
                for n in range(PACK):
                    shift = (n - q) * SG % half
                    moved = gains[n][part]
                    moved = pltpu.roll(moved, shift, axis=1) if shift else moved
                    picked = moved if n == 0 else jnp.where(lane_pack == n, moved, picked)
                gain[part, p, q * rows_at:(q + 1) * rows_at] = picked


def predict_kernel(
    n_stn, n_chan, n_tile,
    x_ref, off_ref, pair_ref, live_ref, beam_hbm, uv_ref, seen_ref, out_ref,
    full, ar, ai, br, bi, cr, ci, dr, di, tab, eu, cuts, inbox,
    beam_ref, beams, gain, dft_x, dft_y, ev, uu, outbox, box,
    z_send, y_send, m_send, recv, cut_send, cut_recv, vis_send, vis_recv, beam_sem,
):
    stn, chan, tile = lax.axis_index("stn"), lax.axis_index("chan"), lax.axis_index("tile")
    tiles, piece_rows, columns = x_ref.shape
    quarter = columns // n_chan
    rows = n_stn * tiles * piece_rows
    group = SUB_TILE * n_tile
    strip_half = TILE_DEV * n_tile * TL // 2
    mate, across = chan ^ 1, chan ^ 2
    hops = [1, n_stn - 1] + list(range(2, n_stn - 1))
    sources = [lax.rem(stn + d, n_stn) for d in hops]

    beam_copy = pltpu.make_async_copy(beam_hbm, beam_ref, beam_sem)
    beam_copy.start()
    barrier = pltpu.get_barrier_semaphore()
    partners = [{"stn": s} for s in sources] + [{"chan": lax.rem(chan + d, n_chan)} for d in range(1, n_chan)]
    partners += [{"tile": lax.rem(tile + d, n_tile)} for d in range(1, n_tile)]
    for where in partners:
        pl.semaphore_signal(barrier, inc=1, device_id=where, device_id_type=MESH)
    pl.semaphore_wait(barrier, len(partners))

    share = tiles // CUTS
    travels = [(s, h) for s in sources for h in range(CUTS)]

    def own(h):
        return x_ref.at[
            pl.ds(h * share, share), :, pl.ds(pl.multiple_of(chan * quarter, quarter), quarter)
        ]

    def piece(c, s, h):
        return full.at[c, s, pl.ds(h * share, share)]

    z_copies = [
        remote(own(h), piece(chan, stn, h), z_send.at[n], recv.at[chan, stn, h], {"stn": s})
        for n, (s, h) in enumerate(travels)
    ]
    for copy in z_copies:
        copy.start()
    for c in range(n_chan):
        full[c, stn] = x_ref[:, :, c * quarter:(c + 1) * quarter]

    first = pl.multiple_of(stn * group, group)
    col_pos = lax.broadcasted_iota(jnp.int32, (8, columns), 1) - columns // 2
    lane = lax.broadcasted_iota(jnp.int32, (8, rows), 1)
    shard = tiles * piece_rows
    row_s = lax.div(lane, shard)
    row_t = lax.div(lax.rem(lane, shard), piece_rows)
    row_pos = (tile * TILE_DEV + row_t) * TL + row_s * piece_rows + lax.rem(lane, piece_rows) - strip_half
    for step in range(SG // 8):
        part = slice(8 * step, 8 * step + 8)
        pixel = lax.broadcasted_iota(jnp.int32, (8, 1), 0) + 8 * step
        br[part], bi[part] = unit_phase(pixel * col_pos)
        dr[part], di[part] = unit_phase(pixel * row_pos)

    @pl.loop(0, group // 8)
    def _(step):
        at = pl.multiple_of(step * 8, 8)
        u_first = jnp.zeros((8, 1), jnp.int32)
        v_first = u_first
        for n in range(8):
            here = iota((8, 1), 0) == n
            u_first = jnp.where(here, off_ref[0, first + at + n], u_first)
            v_first = jnp.where(here, off_ref[1, first + at + n], v_first)
        ar[pl.ds(at, 8)], ai[pl.ds(at, 8)] = unit_phase(v_first * col_pos)
        cr[pl.ds(at, 8)], ci[pl.ds(at, 8)] = unit_phase(u_first * row_pos)

    @pl.loop(0, group // PACK)
    def _(pack):
        base = pl.multiple_of(pack * 2 * PACK * SG, 2 * PACK * SG)
        for n in range(PACK):
            j = pack * PACK + n
            real, imag = cmul(ar[pl.ds(j, 1)], ai[pl.ds(j, 1)], br[...], bi[...])
            tab[pl.ds(base + n * SG, SG)] = real.astype(jnp.bfloat16)
            tab[pl.ds(base + (PACK + n) * SG, SG)] = imag.astype(jnp.bfloat16)
            real, imag = cmul(cr[pl.ds(j, 1)], ci[pl.ds(j, 1)], dr[...], di[...])
            real, imag = real.astype(jnp.bfloat16), imag.astype(jnp.bfloat16)
            eu[pl.ds(base + n * SG, SG), :rows] = real
            eu[pl.ds(base + n * SG, SG), rows:] = -imag
            eu[pl.ds(base + (PACK + n) * SG, SG), :rows] = imag
            eu[pl.ds(base + (PACK + n) * SG, SG), rows:] = real

    onward = []

    def forward(c, n, sems, slot, to):
        s, h = travels[n]
        copy = remote(
            piece(c, s, h), piece(c, s, h), sems.at[slot], recv.at[c, s, h], {"chan": to}
        )
        copy.start()
        onward.append(copy)

    def arrive(c, n, source):
        s, h = travels[n]
        remote(piece(c, s, h), piece(c, s, h), z_send.at[n], recv.at[c, s, h], source).wait_recv()

    def pass_across(n):
        arrive(across, n, {"chan": across})
        forward(across, n, m_send, len(travels) + n, mate)

    for n, (s, h) in enumerate(travels):
        arrive(chan, n, {"stn": s})
        forward(chan, n, y_send, n, across)
        forward(chan, n, m_send, n, mate)
    beam_copy.wait()
    prediction_tables(pair_ref, beam_ref, uv_ref, beams, gain, dft_x, dft_y, ev, uu)
    for n in range(len(travels)):
        pass_across(n)
    for n in range(len(travels)):
        arrive(mate, n, {"chan": mate})
        arrive(mate ^ 2, n, {"chan": mate})
    for copy in z_copies + onward:
        copy.wait_send()

    lane_pack = lax.broadcasted_iota(jnp.int32, (SG, PACK * SG), 1) >> (SG.bit_length() - 1)

    def own_block(half):
        picked = half[:SG]
        for n in range(1, PACK):
            picked = jnp.where(lane_pack == n, half[n * SG:(n + 1) * SG], picked)
        return picked

    packs = SUB_TILE // PACK
    both = 2 * PACK * SG
    half = PACK * SG
    per_step = 2
    sent = []
    for d in range(1, n_tile + 1):
        peer = lax.rem(tile + d, n_tile)

        @pl.loop(0, packs // per_step)
        def _(step):
            pack = peer * packs + step * per_step
            at = pl.multiple_of(pack * both, both)
            q = dot_nt(tab[pl.ds(at, per_step * both), :quarter], full[0].reshape(rows, quarter))
            for c in range(1, n_chan):
                q += dot_nt(
                    tab[pl.ds(at, per_step * both), c * quarter:(c + 1) * quarter],
                    full[c].reshape(rows, quarter),
                )
            q = q.astype(jnp.bfloat16)
            for k in range(per_step):
                top = k * both
                q_k = jnp.concatenate(
                    [q[top:top + both // 2], q[top + both // 2:top + both]], axis=1
                )
                cut = dot_nt(eu[pl.ds(at + top, both)], q_k)
                cuts[pack + k, :SG] = own_block(cut[:both // 2])
                cuts[pack + k, SG:] = own_block(cut[both // 2:])

        if d < n_tile:
            copy = remote(
                cuts.at[pl.ds(peer * packs, packs)], inbox.at[d - 1],
                cut_send.at[d - 1], cut_recv.at[d - 1], {"tile": peer},
            )
            copy.start()
            sent.append(copy)
    total = cuts[pl.ds(tile * packs, packs)]
    for d, copy in enumerate(sent):
        copy.wait()
        total += inbox[d]
    lines = []
    for p in range(packs):
        high, low = split(total[p])
        z = dot_nn(dft_x[...], jnp.concatenate([high, low, high], axis=0))
        lines.append(jnp.concatenate([z[:SG], z[SG:]], axis=1))
    high, low = split(jnp.concatenate(lines, axis=0))
    sub = dot_nn(high, dft_y[0]) + dot_nn(low, dft_y[0]) + dot_nn(high, dft_y[1])
    lane_pair = (iota((SG, both), 1) >> (SG.bit_length() - 1)) & (PACK - 1)
    for p in range(packs):
        sub_p = sub[p * SG:(p + 1) * SG]
        real, imag = cmul(sub_p[:, :half], sub_p[:, half:], gain[0, p], gain[1, p])
        weighted = jnp.concatenate([real, imag], axis=1)
        apart = [jnp.where(lane_pair == n, weighted, 0.0) for n in range(PACK)]
        high, low = split(jnp.concatenate(apart, axis=0))
        inner = dot_nn(high, ev[0, p]) + dot_nn(low, ev[0, p]) + dot_nn(high, ev[1, p])
        real, imag = cmul(uu[0, p], uu[1, p], inner[:, :half], inner[:, half:])
        outbox[:, 0, p] = real.reshape(PACK, SG, half).sum(axis=1)
        outbox[:, 1, p] = imag.reshape(PACK, SG, half).sum(axis=1)

    sent = []
    for d in range(1, n_chan):
        to = lax.rem(chan + d, n_chan)
        copy = remote(
            outbox.at[to], box.at[chan], vis_send.at[d - 1], vis_recv.at[chan], {"chan": to}
        )
        copy.start()
        sent.append(copy)
    box[chan] = outbox[chan]
    for d in range(1, n_chan):
        source = lax.rem(chan + d, n_chan)
        remote(
            outbox.at[source], box.at[source], vis_send.at[d - 1], vis_recv.at[source],
            {"chan": source},
        ).wait_recv()
    for g in range(n_chan):
        at = slice(g * half, (g + 1) * half)
        time_step = lax.rem(iota((1, half), 1) + g * half, TIMES)
        for p in range(packs):
            live = time_step < live_ref[0, p]
            for k in range(2):
                seen = seen_ref[k, p, :, at]
                out_ref[k, p, :, at] = jnp.where(live, seen - box[g, k, p:p + 1], 0.0)
    for copy in sent:
        copy.wait_send()


def predict_call(model_image, offsets, pair_ids, live, station_beams, uv_block, observed):
    n_stn, n_chan, n_tile = (lax.axis_size(a) for a in ("stn", "chan", "tile"))
    tiles, piece_rows, columns = model_image.shape
    rows = n_stn * tiles * piece_rows
    group = SUB_TILE * n_tile
    packs = SUB_TILE // PACK
    f32, bf16 = jnp.float32, jnp.bfloat16
    half = PACK * SG
    assert PACK == n_chan
    vmem = pl.BlockSpec(memory_space=pltpu.VMEM)
    smem = pl.BlockSpec(memory_space=pltpu.SMEM)
    dma = pltpu.SemaphoreType.DMA
    return pl.pallas_call(
        functools.partial(predict_kernel, n_stn, n_chan, n_tile),
        out_shape=jax.ShapeDtypeStruct(observed.shape, f32),
        in_specs=[vmem, smem, smem, smem, pl.BlockSpec(memory_space=pl.ANY), vmem, vmem],
        out_specs=vmem,
        scratch_shapes=[
            pltpu.VMEM((n_chan, n_stn, tiles, piece_rows, columns // n_chan), bf16),
            pltpu.VMEM((group, columns), f32),
            pltpu.VMEM((group, columns), f32),
            pltpu.VMEM((SG, columns), f32),
            pltpu.VMEM((SG, columns), f32),
            pltpu.VMEM((group, rows), f32),
            pltpu.VMEM((group, rows), f32),
            pltpu.VMEM((SG, rows), f32),
            pltpu.VMEM((SG, rows), f32),
            pltpu.VMEM((group * 2 * SG, columns), bf16),
            pltpu.VMEM((group * 2 * SG, 2 * rows), bf16),
            pltpu.VMEM((group // PACK, 2 * SG, PACK * SG), f32),
            pltpu.VMEM((max(n_tile - 1, 1), packs, 2 * SG, PACK * SG), f32),
            pltpu.VMEM(station_beams.shape, f32),
            pltpu.VMEM((2, 2, SUB_TILE, SG // PACK, half), f32),
            pltpu.VMEM((2, packs, SG, half), f32),
            pltpu.VMEM((2 * SG, 6 * SG), bf16),
            pltpu.VMEM((2, 2 * half, 2 * half), bf16),
            pltpu.VMEM((2, packs, 2 * half, 2 * half), bf16),
            pltpu.VMEM((2, packs, half, half), f32),
            pltpu.VMEM((n_chan, 2, packs, half), f32),
            pltpu.VMEM((n_chan, 2, packs, half), f32),
            dma((CUTS * (n_stn - 1),)),
            dma((CUTS * (n_stn - 1),)),
            dma((2 * CUTS * (n_stn - 1),)),
            dma((n_chan, n_stn, CUTS)),
            dma((max(n_tile - 1, 1),)),
            dma((max(n_tile - 1, 1),)),
            dma((n_chan - 1,)),
            dma((n_chan,)),
            pltpu.SemaphoreType.DMA,
        ],
        compiler_params=pltpu.CompilerParams(
            collective_id=0, has_side_effects=True, vmem_limit_bytes=60 * 1024 * 1024
        ),
    )(model_image, offsets.T, pair_ids.T, live.T, station_beams, uv_block, observed)


def on_device(
    model_image,
    station_beams,
    subgrid_offsets,
    subgrid_stations,
    visibility_uv,
    observed,
    live_counts,
):
    return predict_call(
        model_image, subgrid_offsets[0], subgrid_stations, live_counts, station_beams,
        visibility_uv, observed,
    )


def solution(mesh):
    return jax.shard_map(
        on_device,
        mesh=mesh,
        in_specs=(
            P("tile", "stn", None),
            P(),
            P("chan", None, None),
            P(("stn", "tile"), None),
            P(None, ("stn", "tile"), "chan"),
            P(None, ("stn", "tile"), "chan", None),
            P(("stn", "tile"), "chan"),
        ),
        out_specs=P(None, ("stn", "tile"), "chan", None),
        check_vma=False,
    )
```
